32 devices in a mesh: dp: 1 (over z), tp: 32 (over y, x, core).
Axes of the slice: x: 4, y: 4, z: 1, core: 2. Of those that a mesh axis runs over, the one named last changes fastest.
The devices are a block of a 4x4x8 slice.
Arguments:
- x: bfloat16 [2048, 4096], P('dp')
- mu1: float32 [2048], P('dp')
- rs1: float32 [2048], P('dp')
- g1: bfloat16 [4096], replicated
- g2: bfloat16 [4096], replicated
- dy: bfloat16 [2048, 4096], P('dp')
- wqkv: bfloat16 [4096, 12288], P(None, 'tp')
- wo: bfloat16 [32, 128, 4096], P('tp')
- w1: bfloat16 [4096, 16384], P(None, 'tp')
- w2: bfloat16 [16384, 4096], P('tp')
Outputs:
- output 1: bfloat16 [2048, 4096], P('dp')
- output 2: bfloat16 [4096, 12288], P('dp', 'tp')
- output 3: bfloat16 [32, 128, 4096], P(('dp', 'tp'))
- output 4: bfloat16 [4096, 16384], P('dp', 'tp')
- output 5: bfloat16 [16384, 4096], P(('dp', 'tp'))
All inputs are finite; a program needn't handle non-finite values.
Results may differ from the reference program's by a relative error of at most 0.0182407.
Values are sent between devices in bfloat16 or wider.
A program may use at most 768 MiB of HBM per device.

```python
import jax
import jax.numpy as jnp
from jax import lax

T = 2048
D = 4096
HEADS = 32
FF = 16384
HEAD = D // HEADS
EPS = 1.0 / 100000
QK_GAIN = 2.5 ** 0.5


def setup_inputs(seed: int = 0, part: int = 0) -> dict:
    kp = jax.random.fold_in(jax.random.key(seed), part)
    ka = jax.random.split(kp, 4)
    kw = jax.random.split(jax.random.key(seed + 1), 6)
    z = jax.random.normal(ka[0], (T, D), jnp.float32)
    z = z - jnp.mean(z, axis=-1, keepdims=True)
    z = z * lax.rsqrt(jnp.mean(z * z, axis=-1, keepdims=True))
    mu1 = 0.5 * jax.random.normal(ka[1], (T,), jnp.float32)
    rs1 = jax.random.uniform(ka[2], (T,), jnp.float32, 0.7, 1.4)
    x = (mu1[:, None] + z / rs1[:, None]).astype(jnp.bfloat16)
    dy = jax.random.normal(ka[3], (T, D), jnp.float32).astype(jnp.bfloat16)
    g1 = jax.random.uniform(kw[0], (D,), jnp.float32, 0.6, 1.4).astype(jnp.bfloat16)
    g2 = jax.random.uniform(kw[1], (D,), jnp.float32, 0.6, 1.4).astype(jnp.bfloat16)
    gain = jnp.array([QK_GAIN, QK_GAIN, 1.0], jnp.float32)[None, None, :, None]
    wqkv = jax.random.normal(kw[2], (D, HEADS, 3, HEAD), jnp.float32) * gain * D ** -0.5
    wo = jax.random.normal(kw[3], (HEADS, HEAD, D), jnp.float32) * D ** -0.5
    w1 = jax.random.normal(kw[4], (D, FF), jnp.float32) * D ** -0.5
    w2 = jax.random.normal(kw[5], (FF, D), jnp.float32) * FF ** -0.5
    return {"x": x, "mu1": mu1, "rs1": rs1, "g1": g1, "g2": g2, "dy": dy,
            "wqkv": wqkv.reshape(D, 3 * D).astype(jnp.bfloat16), "wo": wo.astype(jnp.bfloat16),
            "w1": w1.astype(jnp.bfloat16), "w2": w2.astype(jnp.bfloat16)}


def _ln_bwd(dn, xh, rs, g):
    u = dn * g
    return rs[:, None] * (u - jnp.mean(u, axis=-1, keepdims=True) - xh * jnp.mean(u * xh, axis=-1, keepdims=True))


def _probs(q, k):
    s = jnp.dot(q, k.T, preferred_element_type=jnp.float32) * HEAD ** -0.5
    mask = jnp.arange(T)[:, None] >= jnp.arange(T)[None, :]
    return jax.nn.softmax(jnp.where(mask, s, -jnp.inf), axis=-1)


def _head_fwd(qkv):
    q, k, v = qkv[:, 0], qkv[:, 1], qkv[:, 2]
    p = _probs(q, k)
    return jnp.dot(p.astype(jnp.bfloat16), v, preferred_element_type=jnp.float32).astype(jnp.bfloat16)


def _head_bwd(args):
    qkv, do = args
    q, k, v = qkv[:, 0], qkv[:, 1], qkv[:, 2]
    p = _probs(q, k)
    dv = jnp.dot(p.astype(jnp.bfloat16).T, do, preferred_element_type=jnp.float32)
    dpm = jnp.dot(do, v.T, preferred_element_type=jnp.float32)
    ds = (p * (dpm - jnp.sum(p * dpm, axis=-1, keepdims=True)) * HEAD ** -0.5).astype(jnp.bfloat16)
    dq = jnp.dot(ds, k, preferred_element_type=jnp.float32)
    dk = jnp.dot(ds.T, q, preferred_element_type=jnp.float32)
    return jnp.stack([dq, dk, dv], axis=1).astype(jnp.bfloat16)


def reference(x, mu1, rs1, g1, g2, dy, wqkv, wo, w1, w2):
    xf = x.astype(jnp.float32)
    g1f = g1.astype(jnp.float32)
    g2f = g2.astype(jnp.float32)
    xh1 = (xf - mu1[:, None]) * rs1[:, None]
    n1 = (xh1 * g1f).astype(jnp.bfloat16)
    qkv = jnp.dot(n1, wqkv, preferred_element_type=jnp.float32).astype(jnp.bfloat16)
    qkv = jnp.moveaxis(qkv.reshape(T, HEADS, 3, HEAD), 1, 0)
    o = lax.map(_head_fwd, qkv)
    o = jnp.moveaxis(o, 0, 1).reshape(T, D)
    wo2 = wo.reshape(D, D)
    h1 = xf + jnp.dot(o, wo2, preferred_element_type=jnp.float32)
    mu2 = jnp.mean(h1, axis=-1, keepdims=True)
    xc = h1 - mu2
    rs2 = lax.rsqrt(jnp.mean(xc * xc, axis=-1) + EPS)
    xh2 = xc * rs2[:, None]
    n2 = (xh2 * g2f).astype(jnp.bfloat16)
    a = jnp.dot(n2, w1, preferred_element_type=jnp.float32)
    gl, gelu_vjp = jax.vjp(jax.nn.gelu, a)
    gb = gl.astype(jnp.bfloat16)
    dw2 = jnp.dot(gb.T, dy, preferred_element_type=jnp.float32).astype(jnp.bfloat16)
    dg = jnp.dot(dy, w2.T, preferred_element_type=jnp.float32)
    da = gelu_vjp(dg)[0].astype(jnp.bfloat16)
    dw1 = jnp.dot(n2.T, da, preferred_element_type=jnp.float32).astype(jnp.bfloat16)
    dn2 = jnp.dot(da, w1.T, preferred_element_type=jnp.float32)
    dh1 = dy.astype(jnp.float32) + _ln_bwd(dn2, xh2, rs2, g2f)
    dh1b = dh1.astype(jnp.bfloat16)
    dwo = jnp.dot(o.T, dh1b, preferred_element_type=jnp.float32).astype(jnp.bfloat16).reshape(HEADS, HEAD, D)
    do = jnp.dot(dh1b, wo2.T, preferred_element_type=jnp.float32).astype(jnp.bfloat16)
    do = jnp.moveaxis(do.reshape(T, HEADS, HEAD), 1, 0)
    dqkv = lax.map(_head_bwd, (qkv, do))
    dqkv = jnp.moveaxis(dqkv, 0, 1).reshape(T, 3 * D)
    dwqkv = jnp.dot(n1.T, dqkv, preferred_element_type=jnp.float32).astype(jnp.bfloat16)
    dn1 = jnp.dot(dqkv, wqkv.T, preferred_element_type=jnp.float32)
    dx = (dh1 + _ln_bwd(dn1, xh1, rs1, g1f)).astype(jnp.bfloat16)
    return dx, dwqkv, dwo, dw1, dw2
```

```python
import functools

import jax
import jax.numpy as jnp
from jax import lax
from jax.experimental import pallas as pl
from jax.experimental.pallas import tpu as pltpu
from jax.sharding import PartitionSpec as P

EPS = 1.0 / 100000
F32 = jnp.float32
BF = jnp.bfloat16
MESH = pl.DeviceIdType.MESH
OFFS = (2, 1, 3, 0)
GOFFS = (0, 3, 1, 2)


def _probs(q, k):
    n = q.shape[0]
    s = jnp.dot(q, k.T, preferred_element_type=F32) * q.shape[1] ** -0.5
    mask = jnp.arange(n)[:, None] >= jnp.arange(n)[None, :]
    return jax.nn.softmax(jnp.where(mask, s, -jnp.inf), axis=-1)


def _head_fwd(qkv):
    q, k, v = qkv[:, 0], qkv[:, 1], qkv[:, 2]
    p = _probs(q, k)
    return jnp.dot(p.astype(BF), v, preferred_element_type=F32).astype(BF)


def _head_bwd(qkv, do):
    q, k, v = qkv[:, 0], qkv[:, 1], qkv[:, 2]
    p = _probs(q, k)
    dv = jnp.dot(p.astype(BF).T, do, preferred_element_type=F32)
    dpm = jnp.dot(do, v.T, preferred_element_type=F32)
    ds = (p * (dpm - jnp.sum(p * dpm, axis=-1, keepdims=True)) * q.shape[1] ** -0.5).astype(BF)
    dq = jnp.dot(ds, k, preferred_element_type=F32)
    dk = jnp.dot(ds.T, q, preferred_element_type=F32)
    return jnp.stack([dq, dk, dv], axis=1).astype(BF)


class _Copy:
    def __init__(self, make):
        self.make = make

    def start(self):
        self.make().start()

    def wait_send(self):
        self.make().wait_send()

    def wait_recv(self):
        self.make().wait_recv()


def _rows(n, step, f):
    @pl.loop(0, n // step)
    def _(i):
        f(pl.ds(pl.multiple_of(i * step, step), step))


def _mid_fwd(total, put, ins, outs):
    x, g2 = ins
    xh_out, rs_out = outs
    n = total.shape[0]

    def f(r):
        h = x[r, :].astype(F32) + total[r, :]
        xc = h - jnp.mean(h, axis=-1, keepdims=True)
        rs = lax.rsqrt(jnp.mean(xc * xc, axis=-1, keepdims=True) + EPS)
        xh = xc * rs
        xh_out[r, :] = xh
        rs_out[r, :] = jnp.broadcast_to(rs, (rs.shape[0], rs_out.shape[1]))
        put(r, (xh * g2[...].astype(F32)).astype(BF))
    _rows(n, 16, f)


def _lnb(dn, xh, rs, g):
    u = dn * g
    return rs * (u - jnp.mean(u, axis=-1, keepdims=True) - xh * jnp.mean(u * xh, axis=-1, keepdims=True))


def _mid_mlp(total, put, ins, outs):
    dy, g2, xh, rs = ins
    (dh_out,) = outs
    n = total.shape[0]

    def f(r):
        dh = dy[r, :].astype(F32) + _lnb(total[r, :], xh[r, :], rs[r, 0:1], g2[...].astype(F32))
        dh_out[r, :] = dh
        put(r, dh.astype(BF))
    _rows(n, 16, f)


def _mid_in(total, put, ins, outs):
    x, g1, mu, rs, dh = ins
    n = total.shape[0]

    def f(r):
        xh = (x[r, :].astype(F32) - mu[r, 0:1]) * rs[r, 0:1]
        dx = dh[r, :] + _lnb(total[r, :], xh, rs[r, 0:1], g1[...].astype(F32))
        put(r, dx.astype(BF))
    _rows(n, 16, f)


def _exchange_kernel(side, trans, mid, n_in, n_out, *refs):
    l_ref, w_ref, wp_ref = refs[:3]
    ins = refs[3:3 + n_in]
    g_ref = refs[3 + n_in]
    outs = refs[4 + n_in:4 + n_in + n_out]
    (lp, pb, ra, rb, q, r2a, r2b, ag, tot,
     sl, s1, r1, s2, r2, gs, gr, hs, hr, ds, dr, os_) = refs[4 + n_in + n_out:]
    n = side
    t, d = ag.shape
    half, unit, b = t // 2, t // (2 * n), t // (2 * n * n)
    hb = b // 2
    me = lax.axis_index("tp")
    c, chip = me % 2, me // 2
    y, x = chip // n, chip % n
    f = (1 - c) * y + c * x
    s = (1 - c) * x + c * y

    def dev(f_, s_):
        return (((1 - c) * f_ + c * s_) * n + (1 - c) * s_ + c * f_) * 2 + c

    fr, fl = dev((f + 1) % n, s), dev((f + n - 1) % n, s)
    sr, sl_ = dev(f, (s + 1) % n), dev(f, (s + n - 1) % n)
    partner = me + 1 - 2 * c

    barrier = pltpu.get_barrier_semaphore()
    for p in (fr, fl, sr, sl_, partner):
        pl.semaphore_signal(barrier, inc=1, device_id={"tp": p}, device_id_type=MESH)
    pl.semaphore_wait(barrier, 5)

    def copy(src, dst, ssem, rsem, to):
        return _Copy(lambda: pltpu.make_async_remote_copy(
            src_ref=src, dst_ref=dst, send_sem=ssem, recv_sem=rsem, device_id={"tp": to}, device_id_type=MESH))

    def blk(k):
        return (f + k) % n

    lx = copy(l_ref.at[pl.ds(pl.multiple_of((1 - c) * half, half), half)], lp, sl.at[0], sl.at[1], partner)
    lx.start()
    lx.wait_recv()

    dims = (((1,), (1,)), ((), ())) if trans else (((1,), (0,)), ((), ()))
    nt = 512

    def product(k):
        sp = (s + OFFS[k]) % n
        own = l_ref[pl.ds(pl.multiple_of(c * half + sp * unit, unit), unit), :]
        oth = lp[pl.ds(pl.multiple_of(sp * unit, unit), unit), :]

        @pl.loop(0, d // nt)
        def _(j):
            cs = pl.ds(pl.multiple_of(j * nt, nt), nt)
            wa = w_ref[cs, :] if trans else w_ref[:, cs]
            wb = wp_ref[cs, :] if trans else wp_ref[:, cs]
            acc = lax.dot_general(own, wa, dims, preferred_element_type=F32)
            acc = acc + lax.dot_general(oth, wb, dims, preferred_element_type=F32)
            acc = acc.astype(BF)
            for i in range(n):
                pb[k, i, :, cs] = acc[i * b:(i + 1) * b]

    def add_rows(dst, src, rows, off):
        @pl.loop(0, rows // 16)
        def _(i):
            rd = pl.ds(pl.multiple_of(off + i * 16, 16), 16)
            rs_ = pl.ds(pl.multiple_of(i * 16, 16), 16)
            dst[rd, :] = (dst[rd, :].astype(F32) + src[rs_, :].astype(F32)).astype(BF)

    def c1a(k):
        o = pb.at[k, blk(2)]
        return (copy(o.at[pl.ds(0, hb)], ra.at[k, 0], s1.at[k, 0], r1.at[k, 0], fr),
                copy(o.at[pl.ds(hb, hb)], ra.at[k, 1], s1.at[k, 1], r1.at[k, 1], fl))

    def c1b(k):
        return (copy(pb.at[k, blk(1)], rb.at[k, 0], s1.at[k, 2], r1.at[k, 2], fr),
                copy(pb.at[k, blk(3)], rb.at[k, 1], s1.at[k, 3], r1.at[k, 3], fl))

    def c2a():
        return (copy(q.at[0, pl.ds(0, hb)], r2a.at[0], s2.at[0], r2.at[0], sr),
                copy(q.at[0, pl.ds(hb, hb)], r2a.at[1], s2.at[1], r2.at[1], sl_))

    def c2b():
        return (copy(q.at[1], r2b.at[0], s2.at[2], r2.at[2], sr),
                copy(q.at[2], r2b.at[1], s2.at[3], r2.at[3], sl_))

    def step_a(k):
        product(k)
        for cp in c1a(k):
            cp.start()

    def step_b(k):
        ca, cb = c1a(k), c1b(k)
        ca[0].wait_recv()
        add_rows(pb.at[k, blk(1)], ra.at[k, 0], hb, 0)
        cb[0].start()
        ca[1].wait_recv()
        add_rows(pb.at[k, blk(3)], ra.at[k, 1], hb, hb)
        cb[1].start()

    def step_c(k):
        for cp in c1b(k):
            cp.wait_recv()
        mine, l, r = pb.at[k, f], rb.at[k, 0], rb.at[k, 1]

        @pl.loop(0, b // 16)
        def _(i):
            rs_ = pl.ds(pl.multiple_of(i * 16, 16), 16)
            v = mine[rs_, :].astype(F32) + l[rs_, :].astype(F32) + r[rs_, :].astype(F32)
            q[k, rs_, :] = v.astype(BF)

    step_a(0)
    step_a(1)
    step_b(0)
    step_a(2)
    step_b(1)
    step_a(3)
    step_b(2)
    step_b(3)
    a2, b2 = c2a(), c2b()
    step_c(0)
    a2[0].start()
    a2[1].start()
    step_c(1)
    a2[0].wait_recv()
    add_rows(q.at[1], r2a.at[0], hb, 0)
    b2[0].start()
    step_c(2)
    a2[1].wait_recv()
    add_rows(q.at[2], r2a.at[1], hb, hb)
    b2[1].start()
    for cp in c1b(3):
        cp.wait_recv()
    b2[0].wait_recv()
    b2[1].wait_recv()

    def final(r):
        tot[r, :] = (pb[3, f, r, :].astype(F32) + rb[3, 0, r, :].astype(F32) + rb[3, 1, r, :].astype(F32)
                     + r2b[0, r, :].astype(F32) + r2b[1, r, :].astype(F32))
    _rows(b, 16, final)

    def row(s_, f_):
        return pl.multiple_of(c * half + s_ * unit + f_ * b, b)

    r0 = row(s, f)

    def put(r, v):
        ag[pl.ds(pl.multiple_of(r0 + r.start, 16), r.size), :] = v
    mid(tot, put, ins, outs)

    def block(row_, off, size):
        return ag.at[pl.ds(pl.multiple_of(row_ + off, hb), size)]

    def gcopy(row_, off, size, ssem, rsem, to):
        return copy(block(row_, off, size), block(row_, off, size), ssem, rsem, to)

    gS = (gcopy(r0, 0, b, gs.at[0], gr.at[0], sr), gcopy(r0, 0, b, gs.at[1], gr.at[1], sl_),
          gcopy(row((s + n - 1) % n, f), 0, hb, gs.at[2], gr.at[2], sr),
          gcopy(row((s + 1) % n, f), hb, hb, gs.at[3], gr.at[3], sl_))

    def urow(u, k):
        return row((s + GOFFS[u]) % n, blk(k))

    def gF(u):
        return (gcopy(urow(u, 0), 0, b, hs.at[u, 0], hr.at[u, 0], fr),
                gcopy(urow(u, 0), 0, b, hs.at[u, 1], hr.at[u, 1], fl),
                gcopy(urow(u, 3), 0, hb, hs.at[u, 2], hr.at[u, 2], fr),
                gcopy(urow(u, 1), hb, hb, hs.at[u, 3], hr.at[u, 3], fl))

    def pair(u, k):
        return gcopy(urow(u, k), 0, b, ds.at[u, k], dr.at[u, k], partner)

    def f1(u):
        g = gF(u)
        g[0].start()
        g[1].start()
        pair(u, 0).start()

    def f2(u):
        g = gF(u)
        g[0].wait_recv()
        g[2].start()
        pair(u, 3).start()
        g[1].wait_recv()
        g[3].start()
        pair(u, 1).start()

    def f3(u):
        g = gF(u)
        g[2].wait_recv()
        g[3].wait_recv()
        pair(u, 2).start()
        out(c * half + ((s + GOFFS[u]) % n) * unit, u).start()

    def out(r_, i):
        sl2 = pl.ds(pl.multiple_of(r_, unit), unit)
        return pltpu.make_async_copy(ag.at[sl2], g_ref.at[sl2], os_.at[i])

    gS[0].start()
    gS[1].start()
    f1(0)
    gS[0].wait_recv()
    gS[2].start()
    f1(1)
    gS[1].wait_recv()
    gS[3].start()
    f1(2)
    f2(0)
    gS[2].wait_recv()
    gS[3].wait_recv()
    f1(3)
    f2(1)
    f3(0)
    f2(2)
    f3(1)
    f2(3)
    f3(2)
    f3(3)

    def theirs(u):
        return (1 - c) * half + ((f + GOFFS[u]) % n) * unit
    for u in range(n):
        for k in range(n):
            pair(u, k).wait_recv()
        out(theirs(u), n + u).start()
    for u in range(n):
        out(c * half + ((s + GOFFS[u]) % n) * unit, u).wait()
        out(theirs(u), n + u).wait()
    lx.wait_send()
    for k in range(n):
        for cp in c1a(k) + c1b(k):
            cp.wait_send()
    for cp in a2 + b2 + gS:
        cp.wait_send()
    for u in range(n):
        for cp in gF(u):
            cp.wait_send()
        for k in range(n):
            pair(u, k).wait_send()


def _exchange(tp, cid, trans, mid, lhs, w, wp, ins, extra):
    side = round((tp // 2) ** 0.5)
    assert side == 4 and side * side * 2 == tp
    n = side
    t, kk = lhs.shape
    d = w.shape[0] if trans else w.shape[1]
    half, b = t // 2, t // tp
    vm = pl.BlockSpec(memory_space=pltpu.VMEM)
    dma = pltpu.SemaphoreType.DMA
    outs = [jax.ShapeDtypeStruct((t, d), BF)] + [jax.ShapeDtypeStruct(s, F32) for s in extra]
    return pl.pallas_call(
        functools.partial(_exchange_kernel, side, trans, mid, len(ins), len(extra)),
        out_shape=outs,
        in_specs=[vm] * (3 + len(ins)),
        out_specs=[pl.BlockSpec(memory_space=pl.ANY)] + [vm] * len(extra),
        scratch_shapes=[
            pltpu.VMEM((half, kk), BF),
            pltpu.VMEM((n, n, b, d), BF),
            pltpu.VMEM((n, 2, b // 2, d), BF),
            pltpu.VMEM((n, 2, b, d), BF),
            pltpu.VMEM((n - 1, b, d), BF),
            pltpu.VMEM((2, b // 2, d), BF),
            pltpu.VMEM((2, b, d), BF),
            pltpu.VMEM((t, d), BF),
            pltpu.VMEM((b, d), F32),
            dma((2,)),
            dma((n, 4)), dma((n, 4)),
            dma((4,)), dma((4,)),
            dma((4,)), dma((4,)),
            dma((n, 4)), dma((n, 4)),
            dma((n, n)), dma((n, n)),
            dma((2 * n,)),
        ],
        compiler_params=pltpu.CompilerParams(collective_id=cid, has_side_effects=True,
                                             vmem_limit_bytes=62 * 1024 * 1024),
        cost_estimate=pl.CostEstimate(flops=2 * t * kk * d * 12, bytes_accessed=t * d * 4, transcendentals=0),
        name=f"exchange{cid}",
    )(lhs, w, wp, *ins)


def solution(mesh):
    tp = mesh.shape["tp"]
    swap = [(i, i + 1 - 2 * (i % 2)) for i in range(tp)]

    def body(x, mu1, rs1, g1, g2, dy, wqkv, wo, w1, w2):
        hl, hd, d = wo.shape
        t = x.shape[0]
        side = round((tp // 2) ** 0.5)
        b = t // tp
        me = lax.axis_index("tp")
        c, chip = me % 2, me // 2
        yy, xx = chip // side, chip % side
        own = c * (t // 2) + ((1 - c) * (xx * side + yy) + c * (yy * side + xx)) * b
        wo2 = wo.reshape(hl * hd, d)
        wo_p = lax.ppermute(wo2, "tp", swap)
        w1_p = lax.ppermute(w1, "tp", swap)
        wqkv_p = lax.ppermute(wqkv, "tp", swap)

        def mine(a):
            return lax.dynamic_slice_in_dim(a, own, b, 0)

        xr, dyr = mine(x), mine(dy)
        mur = jnp.broadcast_to(mine(mu1)[:, None], (b, 128))
        rsr = jnp.broadcast_to(mine(rs1)[:, None], (b, 128))
        g1r, g2r = g1[None, :], g2[None, :]

        xh1 = (x.astype(F32) - mu1[:, None]) * rs1[:, None]
        n1 = (xh1 * g1.astype(F32)).astype(BF)
        qkv = jnp.dot(n1, wqkv, preferred_element_type=F32).astype(BF)
        qkv = jnp.moveaxis(qkv.reshape(t, hl, 3, hd), 1, 0)
        o = jnp.moveaxis(lax.map(_head_fwd, qkv), 0, 1).reshape(t, hl * hd)
        n2, xh2, rs2 = _exchange(tp, 0, False, _mid_fwd, o, wo2, wo_p, [xr, g2r], [(b, d), (b, 128)])
        a = jnp.dot(n2, w1, preferred_element_type=F32)
        gl, gelu_vjp = jax.vjp(jax.nn.gelu, a)
        gb = gl.astype(BF)
        dw2 = jnp.dot(gb.T, dy, preferred_element_type=F32).astype(BF)
        dg = jnp.dot(dy, w2.T, preferred_element_type=F32)
        da = gelu_vjp(dg)[0].astype(BF)
        dw1 = jnp.dot(n2.T, da, preferred_element_type=F32).astype(BF)
        dh1b, dh1 = _exchange(tp, 1, True, _mid_mlp, da, w1, w1_p, [dyr, g2r, xh2, rs2], [(b, d)])
        dwo = jnp.dot(o.T, dh1b, preferred_element_type=F32).astype(BF).reshape(hl, hd, d)
        do = jnp.dot(dh1b, wo2.T, preferred_element_type=F32).astype(BF)
        do = jnp.moveaxis(do.reshape(t, hl, hd), 1, 0)
        dqkv = lax.map(lambda z: _head_bwd(*z), (qkv, do))
        dqkv = jnp.moveaxis(dqkv, 0, 1).reshape(t, 3 * hl * hd)
        dwqkv = jnp.dot(n1.T, dqkv, preferred_element_type=F32).astype(BF)
        (dx,) = _exchange(tp, 2, True, _mid_in, dqkv, wqkv, wqkv_p, [xr, g1r, mur, rsr, dh1], [])
        return dx, dwqkv, dwo, dw1, dw2

    return jax.shard_map(
        body, mesh=mesh,
        in_specs=(P("dp", None), P("dp"), P("dp"), P(None), P(None), P("dp", None),
                  P(None, "tp"), P("tp", None, None), P(None, "tp"), P("tp", None)),
        out_specs=(P("dp", None), P("dp", "tp"), P(("dp", "tp"), None, None), P("dp", "tp"), P(("dp", "tp"), None)),
        check_vma=False)
```

```python
import functools

import jax
import jax.numpy as jnp
from jax import lax
from jax.experimental import pallas as pl
from jax.experimental.pallas import tpu as pltpu
from jax.sharding import PartitionSpec as P

EPS = 1.0 / 100000
F32 = jnp.float32
BF = jnp.bfloat16
MESH = pl.DeviceIdType.MESH
OFFS = (2, 1, 3, 0)
GOFFS = (0, 3, 1, 2)


def _probs(q, k):
    n = q.shape[0]
    s = jnp.dot(q, k.T, preferred_element_type=F32) * q.shape[1] ** -0.5
    mask = jnp.arange(n)[:, None] >= jnp.arange(n)[None, :]
    return jax.nn.softmax(jnp.where(mask, s, -jnp.inf), axis=-1)


def _head_fwd(qkv):
    q, k, v = qkv[:, 0], qkv[:, 1], qkv[:, 2]
    p = _probs(q, k)
    return jnp.dot(p.astype(BF), v, preferred_element_type=F32).astype(BF)


def _head_bwd(qkv, do):
    q, k, v = qkv[:, 0], qkv[:, 1], qkv[:, 2]
    p = _probs(q, k)
    dv = jnp.dot(p.astype(BF).T, do, preferred_element_type=F32)
    dpm = jnp.dot(do, v.T, preferred_element_type=F32)
    ds = (p * (dpm - jnp.sum(p * dpm, axis=-1, keepdims=True)) * q.shape[1] ** -0.5).astype(BF)
    dq = jnp.dot(ds, k, preferred_element_type=F32)
    dk = jnp.dot(ds.T, q, preferred_element_type=F32)
    return jnp.stack([dq, dk, dv], axis=1).astype(BF)


class _Copy:
    def __init__(self, make):
        self.make = make

    def start(self):
        self.make().start()

    def wait_send(self):
        self.make().wait_send()

    def wait_recv(self):
        self.make().wait_recv()


def _rows(n, step, f):
    @pl.loop(0, n // step)
    def _(i):
        f(pl.ds(pl.multiple_of(i * step, step), step))


def _mid_fwd(total, put, ins, outs):
    x, g2 = ins
    xh_out, rs_out = outs
    n = total.shape[0]

    def f(r):
        h = x[r, :].astype(F32) + total[r, :]
        xc = h - jnp.mean(h, axis=-1, keepdims=True)
        rs = lax.rsqrt(jnp.mean(xc * xc, axis=-1, keepdims=True) + EPS)
        xh = xc * rs
        xh_out[r, :] = xh
        rs_out[r, :] = jnp.broadcast_to(rs, (rs.shape[0], rs_out.shape[1]))
        put(r, (xh * g2[...].astype(F32)).astype(BF))
    _rows(n, 16, f)


def _lnb(dn, xh, rs, g):
    u = dn * g
    return rs * (u - jnp.mean(u, axis=-1, keepdims=True) - xh * jnp.mean(u * xh, axis=-1, keepdims=True))


def _mid_mlp(total, put, ins, outs):
    dy, g2, xh, rs = ins
    (dh_out,) = outs
    n = total.shape[0]

    def f(r):
        dh = dy[r, :].astype(F32) + _lnb(total[r, :], xh[r, :], rs[r, 0:1], g2[...].astype(F32))
        dh_out[r, :] = dh
        put(r, dh.astype(BF))
    _rows(n, 16, f)


def _mid_in(total, put, ins, outs):
    x, g1, mu, rs, dh = ins
    n = total.shape[0]

    def f(r):
        xh = (x[r, :].astype(F32) - mu[r, 0:1]) * rs[r, 0:1]
        dx = dh[r, :] + _lnb(total[r, :], xh, rs[r, 0:1], g1[...].astype(F32))
        put(r, dx.astype(BF))
    _rows(n, 16, f)


class _Layout:
    def __init__(self, n, t):
        self.n = n
        self.half, self.unit, self.b = t // 2, t // (2 * n), t // (2 * n * n)
        me = lax.axis_index("tp")
        c, chip = me % 2, me // 2
        y, x = chip // n, chip % n
        self.c = c
        self.f = f = (1 - c) * y + c * x
        self.s = s = (1 - c) * x + c * y

        def dev(f_, s_):
            return (((1 - c) * f_ + c * s_) * n + (1 - c) * s_ + c * f_) * 2 + c
        self.fr, self.fl = dev((f + 1) % n, s), dev((f + n - 1) % n, s)
        self.sr, self.sl = dev(f, (s + 1) % n), dev(f, (s + n - 1) % n)
        self.partner = me + 1 - 2 * c

    def row(self, s_, f_):
        return pl.multiple_of(self.c * self.half + s_ * self.unit + f_ * self.b, self.b)


def _remote(src, dst, ssem, rsem, to):
    return _Copy(lambda: pltpu.make_async_remote_copy(
        src_ref=src, dst_ref=dst, send_sem=ssem, recv_sem=rsem, device_id={"tp": to}, device_id_type=MESH))


def _core(n, trans, R, late, mid, fill, consume, gather):
    L = _Layout(n, R["ag"].shape[0])
    half, unit, b, c, f, s = L.half, L.unit, L.b, L.c, L.f, L.s
    hb = b // 2
    l_ref, lo, lp, w, wp = R["l"], R["lo"], R["lp"], R["wv"], R["wpv"]
    pb, ra, rb, q, r2a, r2b, ag, tot = (R[k] for k in ("pb", "ra", "rb", "q", "r2a", "r2b", "ag", "tot"))
    d = ag.shape[1]
    lsem = R["lsem"]

    first = [pltpu.make_async_copy(R["w"], w, lsem.at[0]), pltpu.make_async_copy(R["wp"], wp, lsem.at[1]),
             pltpu.make_async_copy(l_ref.at[pl.ds(pl.multiple_of(c * half, half), half)], lo, lsem.at[2])]
    late = [pltpu.make_async_copy(R[a], R[z], lsem.at[3 + i]) for i, (a, z) in enumerate(late)]
    for cp in first:
        cp.start()

    barrier = pltpu.get_barrier_semaphore()
    for p in (L.fr, L.fl, L.sr, L.sl, L.partner):
        pl.semaphore_signal(barrier, inc=1, device_id={"tp": p}, device_id_type=MESH)
    pl.semaphore_wait(barrier, 5)

    def blk(k):
        return (f + k) % n

    lx = _remote(l_ref.at[pl.ds(pl.multiple_of((1 - c) * half, half), half)], lp, R["sl"].at[0], R["sl"].at[1], L.partner)
    lx.start()
    for cp in late:
        cp.start()
    for cp in first:
        cp.wait()
    lx.wait_recv()

    dims = (((1,), (1,)), ((), ())) if trans else (((1,), (0,)), ((), ()))
    nt = 512

    def product(k):
        rows = pl.ds(pl.multiple_of(((s + OFFS[k]) % n) * unit, unit), unit)

        @pl.loop(0, d // nt)
        def _(j):
            cs = pl.ds(pl.multiple_of(j * nt, nt), nt)
            wa = w[cs, :] if trans else w[:, cs]
            wb = wp[cs, :] if trans else wp[:, cs]
            acc = lax.dot_general(lo[rows, :], wa, dims, preferred_element_type=F32)
            acc = acc + lax.dot_general(lp[rows, :], wb, dims, preferred_element_type=F32)
            acc = acc.astype(BF)
            for i in range(n):
                pb[k, i, :, cs] = acc[i * b:(i + 1) * b]

    def add_rows(dst, src, rows, off):
        @pl.loop(0, rows // 16)
        def _(i):
            rd = pl.ds(pl.multiple_of(off + i * 16, 16), 16)
            rs_ = pl.ds(pl.multiple_of(i * 16, 16), 16)
            dst[rd, :] = (dst[rd, :].astype(F32) + src[rs_, :].astype(F32)).astype(BF)

    s1, r1, s2, r2 = R["s1"], R["r1"], R["s2"], R["r2"]

    def c1a(k):
        o = pb.at[k, blk(2)]
        return (_remote(o.at[pl.ds(0, hb)], ra.at[k, 0], s1.at[k, 0], r1.at[k, 0], L.fr),
                _remote(o.at[pl.ds(hb, hb)], ra.at[k, 1], s1.at[k, 1], r1.at[k, 1], L.fl))

    def c1b(k):
        return (_remote(pb.at[k, blk(1)], rb.at[k, 0], s1.at[k, 2], r1.at[k, 2], L.fr),
                _remote(pb.at[k, blk(3)], rb.at[k, 1], s1.at[k, 3], r1.at[k, 3], L.fl))

    a2 = (_remote(q.at[0, pl.ds(0, hb)], r2a.at[0], s2.at[0], r2.at[0], L.sr),
          _remote(q.at[0, pl.ds(hb, hb)], r2a.at[1], s2.at[1], r2.at[1], L.sl))
    b2 = (_remote(q.at[1], r2b.at[0], s2.at[2], r2.at[2], L.sr),
          _remote(q.at[2], r2b.at[1], s2.at[3], r2.at[3], L.sl))

    def step_a(k):
        product(k)
        for cp in c1a(k):
            cp.start()

    def step_b(k):
        ca, cb = c1a(k), c1b(k)
        ca[0].wait_recv()
        add_rows(pb.at[k, blk(1)], ra.at[k, 0], hb, 0)
        cb[0].start()
        ca[1].wait_recv()
        add_rows(pb.at[k, blk(3)], ra.at[k, 1], hb, hb)
        cb[1].start()

    def step_c(k):
        for cp in c1b(k):
            cp.wait_recv()
        mine, l, r = pb.at[k, f], rb.at[k, 0], rb.at[k, 1]

        @pl.loop(0, b // 16)
        def _(i):
            rs_ = pl.ds(pl.multiple_of(i * 16, 16), 16)
            v = mine[rs_, :].astype(F32) + l[rs_, :].astype(F32) + r[rs_, :].astype(F32)
            q[k, rs_, :] = v.astype(BF)

    step_a(0)
    step_a(1)
    step_b(0)
    step_a(2)
    step_b(1)
    step_a(3)
    for cp in late:
        cp.wait()
    fill(0)
    step_b(2)
    step_c(0)
    a2[0].start()
    a2[1].start()
    fill(1)
    step_b(3)
    step_c(1)
    a2[0].wait_recv()
    add_rows(q.at[1], r2a.at[0], hb, 0)
    b2[0].start()
    fill(2)
    step_c(2)
    a2[1].wait_recv()
    add_rows(q.at[2], r2a.at[1], hb, hb)
    b2[1].start()
    fill(3)
    for cp in c1b(3):
        cp.wait_recv()
    b2[0].wait_recv()
    b2[1].wait_recv()

    def final(r):
        tot[r, :] = (pb[3, f, r, :].astype(F32) + rb[3, 0, r, :].astype(F32) + rb[3, 1, r, :].astype(F32)
                     + r2b[0, r, :].astype(F32) + r2b[1, r, :].astype(F32))
    _rows(b, 16, final)

    r0 = L.row(s, f)

    def put(r, v):
        ag[pl.ds(pl.multiple_of(r0 + r.start, 16), r.size), :] = v
    mid(tot, put)

    gs, gr, hs, hr, ds, dr, osem = (R[k] for k in ("gs", "gr", "hs", "hr", "ds", "dr", "osem"))

    def gcopy(row_, off, size, ssem, rsem, to):
        v = ag.at[pl.ds(pl.multiple_of(row_ + off, hb), size)]
        return _remote(v, v, ssem, rsem, to)

    gS = (gcopy(r0, 0, b, gs.at[0], gr.at[0], L.sr), gcopy(r0, 0, b, gs.at[1], gr.at[1], L.sl),
          gcopy(L.row((s + n - 1) % n, f), 0, hb, gs.at[2], gr.at[2], L.sr),
          gcopy(L.row((s + 1) % n, f), hb, hb, gs.at[3], gr.at[3], L.sl))

    def urow(u, k):
        return L.row((s + GOFFS[u]) % n, blk(k))

    def gF(u):
        return (gcopy(urow(u, 0), 0, b, hs.at[u, 0], hr.at[u, 0], L.fr),
                gcopy(urow(u, 0), 0, b, hs.at[u, 1], hr.at[u, 1], L.fl),
                gcopy(urow(u, 3), 0, hb, hs.at[u, 2], hr.at[u, 2], L.fr),
                gcopy(urow(u, 1), hb, hb, hs.at[u, 3], hr.at[u, 3], L.fl))

    def pair(u, k):
        return gcopy(urow(u, k), 0, b, ds.at[u, k], dr.at[u, k], L.partner)

    def urows(u, i):
        core = c + i * (1 - 2 * c)
        return core * half + (((1 - i) * s + i * f + GOFFS[u]) % n) * unit

    def out(u, i):
        sl2 = pl.ds(pl.multiple_of(urows(u, i), unit), unit)
        return pltpu.make_async_copy(ag.at[sl2], R["g"].at[sl2], osem.at[2 * u + i])

    def f1(u):
        g = gF(u)
        g[0].start()
        g[1].start()
        pair(u, 0).start()

    def f2(u):
        g = gF(u)
        g[0].wait_recv()
        g[2].start()
        pair(u, 3).start()
        g[1].wait_recv()
        g[3].start()
        pair(u, 1).start()

    def f3(u):
        g = gF(u)
        g[2].wait_recv()
        g[3].wait_recv()
        pair(u, 2).start()
        if gather:
            out(u, 0).start()

    def use(u):
        for k in range(n):
            pair(u, k).wait_recv()
        if gather:
            out(u, 1).start()
        consume(u, lambda i: pl.multiple_of(urows(u, i), unit))

    gS[0].start()
    gS[1].start()
    f1(0)
    gS[0].wait_recv()
    gS[2].start()
    f1(1)
    gS[1].wait_recv()
    gS[3].start()
    f1(2)
    f2(0)
    gS[2].wait_recv()
    gS[3].wait_recv()
    f1(3)
    f2(1)
    f3(0)
    use(0)
    f2(2)
    f3(1)
    use(1)
    f2(3)
    f3(2)
    use(2)
    f3(3)
    use(3)

    if gather:
        for u in range(n):
            out(u, 0).wait()
            out(u, 1).wait()
    lx.wait_send()
    for k in range(n):
        for cp in c1a(k) + c1b(k):
            cp.wait_send()
    for cp in a2 + b2 + gS:
        cp.wait_send()
    for u in range(n):
        for cp in gF(u):
            cp.wait_send()
        for k in range(n):
            pair(u, k).wait_send()


class _Stream:
    def __init__(self, srcs, factor, out, buf, stage, isem, osem, cuts):
        self.srcs, self.factor, self.out, self.buf, self.stage = srcs, factor, out, buf, stage
        self.isem, self.osem, self.cuts = isem, osem, cuts
        self.width = buf.shape[2]
        self.per = srcs[0].shape[1] // self.width
        self.n = self.per * len(srcs)
        assert cuts[-1] == self.n

    def load(self, i, go):
        sl = i % 2
        for a, src in enumerate(self.srcs):
            @pl.when(jnp.logical_and(i >= a * self.per, i < (a + 1) * self.per))
            def _():
                cs = pl.ds(pl.multiple_of((i - a * self.per) * self.width, self.width), self.width)
                go(pltpu.make_async_copy(src.at[:, cs], self.buf.at[sl], self.isem.at[sl]))

    def store(self, i):
        cs = pl.ds(pl.multiple_of((i % self.per) * self.width, self.width), self.width)
        return pltpu.make_async_copy(self.stage.at[i % 2], self.out.at[i // self.per, :, cs], self.osem.at[i % 2])

    def fill(self, site):
        lo, hi = ((0,) + self.cuts)[site], self.cuts[site]
        if site == 0:
            self.load(jnp.int32(0), lambda cp: cp.start())

        @pl.loop(lo, hi)
        def _(i):
            self.load(i, lambda cp: cp.wait())

            @pl.when(i + 1 < self.n)
            def _():
                self.load(i + 1, lambda cp: cp.start())

            @pl.when(i >= 2)
            def _():
                self.store(i - 2).wait()
            v = jnp.dot(self.factor[i // self.per], self.buf[i % 2], preferred_element_type=F32)
            self.stage[i % 2] = v.astype(BF)
            self.store(i).start()
        if hi == self.n:
            self.store(jnp.int32(self.n - 2)).wait()
            self.store(jnp.int32(self.n - 1)).wait()


_K = 0.7978845608028654


def _fwd_kernel(names, n, *refs):
    R = dict(zip(names, refs))
    dgs, dyb, dsem, osem2 = R["dgs"], R["dyb"], R["dsem"], R["lsem2"]
    rows = dyb.shape[1]
    tiles = dgs.shape[0] // rows
    cuts = (2, 5, 7, tiles)

    def load(i):
        return pltpu.make_async_copy(R["dy"].at[pl.ds(pl.multiple_of(i * rows, rows), rows)], dyb.at[i % 2], dsem.at[i % 2])

    def fill(site):
        if site == 0:
            load(jnp.int32(0)).start()

        @pl.loop(((0,) + cuts)[site], cuts[site])
        def _(i):
            load(i).wait()

            @pl.when(i + 1 < tiles)
            def _():
                load(i + 1).start()
            dgs[pl.ds(pl.multiple_of(i * rows, rows), rows), :] = lax.dot_general(
                dyb[i % 2], R["w2v"][...], (((1,), (1,)), ((), ())), preferred_element_type=F32)

    def stores(i, r, w):
        return [pltpu.make_async_copy(R["sda"].at[i], R["da"].at[pl.ds(r, w)], osem2.at[0, i]),
                pltpu.make_async_copy(R["sgt"].at[i], R["lt"].at[0, :, pl.ds(r, w)], osem2.at[1, i]),
                pltpu.make_async_copy(R["sdt"].at[i], R["lt"].at[1, :, pl.ds(r, w)], osem2.at[2, i])]
    prev = []

    def consume(u, row):
        w = R["sda"].shape[1]

        @pl.loop(0, 2)
        def _(i):
            r = row(i)
            for p in prev[-1:]:
                for cp in stores(i, p(i), w):
                    cp.wait()
            a = jnp.dot(R["ag"][pl.ds(r, w), :], R["w1v"][...], preferred_element_type=F32)
            th = jnp.tanh(_K * (a + 0.044715 * (a * a * a)))
            cdf = 0.5 * (1.0 + th)
            slope = cdf + 0.5 * a * ((1.0 - th * th) * (_K * (1.0 + (3 * 0.044715) * (a * a))))
            gl = (a * cdf).astype(BF)
            da = (dgs[pl.ds(r, w), :] * slope).astype(BF)
            R["sda"][i] = da
            R["sgt"][i] = gl.T
            R["sdt"][i] = da.T
            for cp in stores(i, r, w):
                cp.start()
        prev.append(row)

    _core(n, False, R, (("w2", "w2v"), ("w1", "w1v")),
          lambda tot, put: _mid_fwd(tot, put, (R["x"], R["g"+"2"]), (R["xh"], R["rs"])), fill, consume, True)
    for i in range(2):
        for cp in stores(i, prev[-1](i), R["sda"].shape[1]):
            cp.wait()


def _mlp_kernel(names, n, *refs):
    R = dict(zip(names, refs))
    st = _Stream((R["dy"], R["n2"]), R["ltv"], R["dw"], R["buf"], R["stage"], R["bsem"], R["tsem"], (6, 18, 26, 32))
    acc = R["acc"]
    d = acc.shape[1]
    w = R["ag"].shape[0] // (2 * n)
    nt = 512

    def consume(u, row):
        @pl.loop(0, 2)
        def _(i):
            r = row(i)
            do = lax.dot_general(R["ag"][pl.ds(r, w), :], R["wv0"][...], (((1,), (1,)), ((), ())), preferred_element_type=F32)
            R["do"][pl.ds(r, w), :] = do.astype(BF)
            ot = R["ov"][pl.ds(r, w), :]

            @pl.loop(0, d // nt)
            def _(j):
                cs = pl.ds(pl.multiple_of(j * nt, nt), nt)
                v = lax.dot_general(ot, R["ag"][pl.ds(r, w), cs], (((0,), (0,)), ((), ())), preferred_element_type=F32)
                acc[:, cs] = acc[:, cs] + v

    acc[...] = jnp.zeros_like(acc)
    _core(n, True, R, (("lt", "ltv"), ("wo", "wv0"), ("o", "ov")),
          lambda tot, put: _mid_mlp(tot, put, (R["dyr"], R["g2"], R["xh"], R["rs"]), (R["dh"],)), st.fill, consume, False)
    R["dwo"][...] = acc[...].astype(BF)


def _in_kernel(names, n, *refs):
    R = dict(zip(names, refs))
    st = _Stream((R["n1"],), R["ltv"], R["dw"], R["buf"], R["stage"], R["bsem"], R["tsem"], (4, 10, 13, 16))
    _core(n, True, R, (("lt", "ltv"),),
          lambda tot, put: _mid_in(tot, put, (R["x"], R["g1"], R["mu"], R["rs"], R["dh"]), ()), st.fill,
          lambda u, row: None, True)


ANY, VM = pl.BlockSpec(memory_space=pl.ANY), pl.BlockSpec(memory_space=pltpu.VMEM)


def _exchange(tp, cid, kernel, flops, ins, outs, scratch):
    n = round((tp // 2) ** 0.5)
    assert n == 4 and n * n * 2 == tp
    l, w, wp = (ins[k][0] for k in ("l", "w", "wp"))
    t, kk = l.shape
    d = w.shape[0] * w.shape[1] // kk
    half, b = t // 2, t // tp
    dma = pltpu.SemaphoreType.DMA
    vm = pltpu.VMEM
    scratch = dict(
        lo=vm((half, kk), BF), lp=vm((half, kk), BF), wv=vm(w.shape, BF), wpv=vm(w.shape, BF),
        pb=vm((n, n, b, d), BF), ra=vm((n, 2, b // 2, d), BF), rb=vm((n, 2, b, d), BF), q=vm((n - 1, b, d), BF),
        r2a=vm((2, b // 2, d), BF), r2b=vm((2, b, d), BF), ag=vm((t, d), BF), tot=vm((b, d), F32),
        lsem=dma((6,)), sl=dma((2,)), s1=dma((n, 4)), r1=dma((n, 4)), s2=dma((4,)), r2=dma((4,)),
        gs=dma((4,)), gr=dma((4,)), hs=dma((n, 4)), hr=dma((n, 4)), ds=dma((n, n)), dr=dma((n, n)), osem=dma((2 * n,)),
        **scratch)
    names = (*ins, *outs, *scratch)
    assert len(set(names)) == len(names)
    return pl.pallas_call(
        functools.partial(kernel, names, n),
        out_shape=[jax.ShapeDtypeStruct(s, dt) for s, dt, _ in outs.values()],
        in_specs=[sp for _, sp in ins.values()],
        out_specs=[sp for _, _, sp in outs.values()],
        scratch_shapes=list(scratch.values()),
        compiler_params=pltpu.CompilerParams(collective_id=cid, has_side_effects=True,
                                             vmem_limit_bytes=67043328),
        cost_estimate=pl.CostEstimate(flops=flops, bytes_accessed=t * d * 4, transcendentals=0),
        name=f"exchange{cid}",
    )(*(a for a, _ in ins.values()))


def _qkv_kernel(x, mu, rs, g, w, n1, qkv):
    v = ((x[...].astype(F32) - mu[...]) * rs[...] * g[...].astype(F32)).astype(BF)
    n1[...] = v
    qkv[...] = jnp.dot(v, w[...], preferred_element_type=F32).astype(BF)


def _norm_qkv(x, mu, rs, g, w):
    t, d = x.shape
    m, rows = w.shape[1], 256
    return pl.pallas_call(
        _qkv_kernel,
        grid=(t // rows,),
        in_specs=[pl.BlockSpec((rows, d), lambda i: (i, 0)), pl.BlockSpec((rows, 1), lambda i: (i, 0)),
                  pl.BlockSpec((rows, 1), lambda i: (i, 0)), pl.BlockSpec((1, d), lambda i: (0, 0)),
                  pl.BlockSpec((d, m), lambda i: (0, 0))],
        out_specs=[pl.BlockSpec((rows, d), lambda i: (i, 0)), pl.BlockSpec((rows, m), lambda i: (i, 0))],
        out_shape=[jax.ShapeDtypeStruct((t, d), BF), jax.ShapeDtypeStruct((t, m), BF)],
        compiler_params=pltpu.CompilerParams(vmem_limit_bytes=40 * 1024 * 1024),
        cost_estimate=pl.CostEstimate(flops=2 * t * d * m, bytes_accessed=t * d * 4, transcendentals=0),
        name="norm_qkv",
    )(x, mu[:, None], rs[:, None], g, w)


def solution(mesh):
    tp = mesh.shape["tp"]
    swap = [(i, i + 1 - 2 * (i % 2)) for i in range(tp)]

    def body(x, mu1, rs1, g1, g2, dy, wqkv, wo, w1, w2):
        hl, hd, d = wo.shape
        t = x.shape[0]
        side = round((tp // 2) ** 0.5)
        b = t // tp
        me = lax.axis_index("tp")
        c, chip = me % 2, me // 2
        yy, xx = chip // side, chip % side
        own = c * (t // 2) + ((1 - c) * (xx * side + yy) + c * (yy * side + xx)) * b
        wo2 = wo.reshape(hl * hd, d)
        wo_p = lax.ppermute(wo2, "tp", swap)
        w1_p = lax.ppermute(w1, "tp", swap)
        wqkv_p = lax.ppermute(wqkv, "tp", swap)

        def mine(a):
            return lax.dynamic_slice_in_dim(a, own, b, 0)

        xr, dyr = mine(x), mine(dy)
        mur = jnp.broadcast_to(mine(mu1)[:, None], (b, 128))
        rsr = jnp.broadcast_to(mine(rs1)[:, None], (b, 128))
        g1r, g2r = g1[None, :], g2[None, :]

        dma, vm = pltpu.SemaphoreType.DMA, pltpu.VMEM
        n1, qkv = _norm_qkv(x, mu1, rs1, g1r, wqkv)
        assert hl == 1
        qkv = qkv.reshape(t, 3, hd)
        o = _head_fwd(qkv)
        m = w1.shape[1]
        unit = t // (2 * side)
        n2, xh2, rs2, da, lt = _exchange(
            tp, 0, _fwd_kernel, 8 * t * d * m,
            dict(l=(o, ANY), w=(wo2, ANY), wp=(wo_p, ANY), x=(xr, VM), g2=(g2r, VM),
                 dy=(dy, ANY), w2=(w2, ANY), w1=(w1, ANY)),
            dict(g=((t, d), BF, ANY), xh=((b, d), F32, VM), rs=((b, 128), F32, VM),
                 da=((t, m), BF, ANY), lt=((2, m, t), BF, ANY)),
            dict(w2v=vm(w2.shape, BF), w1v=vm(w1.shape, BF), dgs=vm((t, m), F32), dyb=vm((2, unit, d), BF),
                 sda=vm((2, unit, m), BF), sgt=vm((2, m, unit), BF), sdt=vm((2, m, unit), BF),
                 dsem=dma((2,)), lsem2=dma((3, 2))))
        dh1, dw, do, dwo = _exchange(
            tp, 1, _mlp_kernel, 8 * t * d * m,
            dict(l=(da, ANY), w=(w1, ANY), wp=(w1_p, ANY), dyr=(dyr, VM), g2=(g2r, VM), xh=(xh2, VM), rs=(rs2, VM),
                 dy=(dy, ANY), n2=(n2, ANY), lt=(lt, ANY), wo=(wo2, ANY), o=(o, ANY)),
            dict(dh=((b, d), F32, VM), dw=((2, m, d), BF, ANY), do=((t, hd), BF, VM), dwo=((hd, d), BF, VM)),
            dict(ltv=vm(lt.shape, BF), wv0=vm(wo2.shape, BF), ov=vm(o.shape, BF), acc=vm((hd, d), F32),
                 buf=vm((2, t, 256), BF), stage=vm((2, m, 256), BF), bsem=dma((2,)), tsem=dma((2,))))
        dw2, dw1 = dw[0], dw[1].T
        dwo = dwo.reshape(hl, hd, d)
        dqkv = _head_bwd(qkv, do).reshape(t, 3 * hd)
        lt2 = dqkv.T[None]
        dx, dwt = _exchange(
            tp, 2, _in_kernel, 8 * t * d * m,
            dict(l=(dqkv, ANY), w=(wqkv, ANY), wp=(wqkv_p, ANY), x=(xr, VM), g1=(g1r, VM), mu=(mur, VM), rs=(rsr, VM),
                 dh=(dh1, VM), n1=(n1, ANY), lt=(lt2, ANY)),
            dict(g=((t, d), BF, ANY), dw=((1, 3 * hd, d), BF, ANY)),
            dict(ltv=vm(lt2.shape, BF), buf=vm((2, t, 256), BF), stage=vm((2, 3 * hd, 256), BF),
                 bsem=dma((2,)), tsem=dma((2,))))
        dwqkv = dwt[0].T
        return dx, dwqkv, dwo, dw1, dw2

    return jax.shard_map(
        body, mesh=mesh,
        in_specs=(P("dp", None), P("dp"), P("dp"), P(None), P(None), P("dp", None),
                  P(None, "tp"), P("tp", None, None), P(None, "tp"), P("tp", None)),
        out_specs=(P("dp", None), P("dp", "tp"), P(("dp", "tp"), None, None), P("dp", "tp"), P(("dp", "tp"), None)),
        check_vma=False)
```

```python
import functools

import jax
import jax.numpy as jnp
from jax import lax
from jax.experimental import pallas as pl
from jax.experimental.pallas import tpu as pltpu
from jax.sharding import PartitionSpec as P

EPS = 1.0 / 100000
F32 = jnp.float32
BF = jnp.bfloat16
MESH = pl.DeviceIdType.MESH
OFFS = (2, 1, 3, 0)
GOFFS = (0, 3, 1, 2)
NN = (((1,), (0,)), ((), ()))
NT = (((1,), (1,)), ((), ()))
TN = (((0,), (0,)), ((), ()))
STEP = 16
LIMIT = 40 * 1024 * 1024


def _down(i):
    return (i, 0)


def _across(i):
    return (0, i)


def _run(plan, **ops):
    for op, k in zip(plan[::2], plan[1::2]):
        ops[op](int(k))


def _causal(i, j, rows, cols):
    q = lax.broadcasted_iota(jnp.int32, (rows, cols), 0) + i * rows
    k = lax.broadcasted_iota(jnp.int32, (rows, cols), 1) + j * cols
    return q >= k


def _scores(q, k, scale):
    return lax.dot_general(q, k, NT, preferred_element_type=F32) * scale


def _lanes(op, v, acc):
    for g in range(v.shape[1] // 128):
        acc = op(acc, v[:, g * 128:(g + 1) * 128])
    return acc


def _attn_fwd_kernel(q_ref, k_ref, v_ref, o_ref, lse_ref, sc):
    i = pl.program_id(0)
    rows, hd = q_ref.shape
    cols = 512
    nb = (i * rows) // cols + 1
    q = q_ref[...]

    def sl(j):
        return pl.ds(pl.multiple_of(j * cols, cols), cols)

    def score(j, m):
        s = _scores(q, k_ref[sl(j), :], hd ** -0.5)
        s = jnp.where(_causal(i, j, rows, cols), s, -1e30)
        sc[:, sl(j)] = s
        return _lanes(jnp.maximum, s, m)
    m = lax.fori_loop(0, nb, score, jnp.full((rows, 128), -1e30, F32))
    m = jnp.max(m, axis=-1, keepdims=True)

    def expo(j, l):
        e = jnp.exp(sc[:, sl(j)] - m)
        sc[:, sl(j)] = e
        return _lanes(jnp.add, e, l)
    l = lax.fori_loop(0, nb, expo, jnp.zeros((rows, 128), F32))
    l = jnp.sum(l, axis=-1, keepdims=True)
    inv = 1.0 / l

    def pv(j, acc):
        p = (sc[:, sl(j)] * inv).astype(BF)
        return acc + jnp.dot(p, v_ref[sl(j), :], preferred_element_type=F32)
    o_ref[...] = lax.fori_loop(0, nb, pv, jnp.zeros((rows, hd), F32)).astype(BF)
    lse_ref[...] = jnp.broadcast_to(m + jnp.log(l), lse_ref.shape)


def _attn_fwd(qkv, hd):
    t = qkv.shape[0]
    rows = 512
    whole = [pl.BlockSpec((t, hd), lambda i, c=c: (0, c)) for c in (1, 2)]
    return pl.pallas_call(
        _attn_fwd_kernel,
        grid=(t // rows,),
        in_specs=[pl.BlockSpec((rows, hd), _down), *whole],
        out_specs=[pl.BlockSpec((rows, hd), _down), pl.BlockSpec((rows, 128), _down)],
        out_shape=[jax.ShapeDtypeStruct((t, hd), BF), jax.ShapeDtypeStruct((t, 128), F32)],
        scratch_shapes=[pltpu.VMEM((rows, t), F32)],
        compiler_params=pltpu.CompilerParams(vmem_limit_bytes=LIMIT),
        cost_estimate=pl.CostEstimate(flops=4 * t * t * hd, bytes_accessed=t * hd * 10, transcendentals=t * t),
        name="attn_fwd",
    )(qkv, qkv, qkv)


def _attn_bwd_kernel(q_ref, k_ref, v_ref, do_ref, lse_ref, dw_ref, dwo_ref, dqkv, dqkvt, dw2, dw1, dwo, ps, dps, dk, dv):
    i = pl.program_id(0)
    rows, hd = q_ref.shape
    cols = 512
    scale = hd ** -0.5
    nb = (i * rows) // cols + 1
    q, do, lse = q_ref[...], do_ref[...], lse_ref[:, 0:1]
    dw2[...] = dw_ref[0]
    dw1[...] = dw_ref[1].T
    dwo[...] = dwo_ref[...]
    ta = TN

    @pl.when(i == 0)
    def _():
        dk[...] = jnp.zeros_like(dk)
        dv[...] = jnp.zeros_like(dv)

    def sl(j):
        return pl.ds(pl.multiple_of(j * cols, cols), cols)

    def first(j, acc):
        s = jnp.where(_causal(i, j, rows, cols), _scores(q, k_ref[sl(j), :], scale), -1e30)
        p = jnp.exp(s - lse)
        dp = _scores(do, v_ref[sl(j), :], 1.0)
        ps[:, sl(j)] = p
        dps[:, sl(j)] = dp
        dv[sl(j), :] = dv[sl(j), :] + lax.dot_general(p.astype(BF), do, ta, preferred_element_type=F32)
        return _lanes(jnp.add, p * dp, acc)
    rsum = jnp.sum(lax.fori_loop(0, nb, first, jnp.zeros((rows, 128), F32)), axis=-1, keepdims=True)

    def second(j, acc):
        ds = (ps[:, sl(j)] * (dps[:, sl(j)] - rsum) * scale).astype(BF)
        dk[sl(j), :] = dk[sl(j), :] + lax.dot_general(ds, q, ta, preferred_element_type=F32)
        return acc + jnp.dot(ds, k_ref[sl(j), :], preferred_element_type=F32)
    dq = lax.fori_loop(0, nb, second, jnp.zeros((rows, hd), F32)).astype(BF)
    rs = pl.ds(pl.multiple_of(i * rows, rows), rows)
    dqkv[rs, 0:hd] = dq
    dqkvt[0, 0:hd, rs] = dq.T

    @pl.when(i == pl.num_programs(0) - 1)
    def _():
        for h, g in ((1, dk), (2, dv)):
            w = g[...].astype(BF)
            dqkv[:, h * hd:(h + 1) * hd] = w
            dqkvt[0, h * hd:(h + 1) * hd, :] = w.T


def _attn_bwd(qkv, do, lse, dw, dwo, hd):
    t = qkv.shape[0]
    rows = 512
    n = t // rows
    m, d = dw.shape[1:]
    w = d // n
    whole = [pl.BlockSpec((t, hd), lambda i, c=c: (0, c)) for c in (1, 2)]
    return pl.pallas_call(
        _attn_bwd_kernel,
        grid=(n,),
        in_specs=[pl.BlockSpec((rows, hd), _down), *whole,
                  pl.BlockSpec((rows, hd), _down), pl.BlockSpec((rows, 128), _down),
                  pl.BlockSpec((2, m, w), lambda i: (0, 0, i)), pl.BlockSpec((hd, w), _across)],
        out_specs=[pl.BlockSpec((t, 3 * hd), lambda i: (0, 0)), pl.BlockSpec((1, 3 * hd, t), lambda i: (0, 0, 0)),
                   pl.BlockSpec((m, w), _across), pl.BlockSpec((w, m), _down),
                   pl.BlockSpec((hd, w), _across)],
        out_shape=[jax.ShapeDtypeStruct((t, 3 * hd), BF), jax.ShapeDtypeStruct((1, 3 * hd, t), BF),
                   jax.ShapeDtypeStruct((m, d), BF), jax.ShapeDtypeStruct((d, m), BF), jax.ShapeDtypeStruct((hd, d), BF)],
        scratch_shapes=[pltpu.VMEM((rows, t), F32), pltpu.VMEM((rows, t), F32),
                        pltpu.VMEM((t, hd), F32), pltpu.VMEM((t, hd), F32)],
        compiler_params=pltpu.CompilerParams(vmem_limit_bytes=LIMIT),
        cost_estimate=pl.CostEstimate(flops=10 * t * t * hd, bytes_accessed=16 * m * d, transcendentals=t * t),
        name="attn_bwd",
    )(qkv, qkv, qkv, do, lse, dw, dwo)


def _finish_kernel(dx_ref, dw_ref, dx, dw):
    dx[...] = dx_ref[...]
    dw[...] = dw_ref[0].T


def _finish(dx, dwt):
    t, d = dx.shape
    m = dwt.shape[1]
    n = 16
    return pl.pallas_call(
        _finish_kernel,
        grid=(n,),
        in_specs=[pl.BlockSpec((t // n, d), _down), pl.BlockSpec((1, m, d // n), lambda i: (0, 0, i))],
        out_specs=[pl.BlockSpec((t // n, d), _down), pl.BlockSpec((d // n, m), _down)],
        out_shape=[jax.ShapeDtypeStruct((t, d), BF), jax.ShapeDtypeStruct((d, m), BF)],
        compiler_params=pltpu.CompilerParams(vmem_limit_bytes=LIMIT),
        cost_estimate=pl.CostEstimate(flops=t * d, bytes_accessed=4 * t * d, transcendentals=0),
        name="finish",
    )(dx, dwt)


class _Copy:
    def __init__(self, make):
        self.make = make

    def start(self):
        self.make().start()

    def wait_send(self):
        self.make().wait_send()

    def wait_recv(self):
        self.make().wait_recv()


def _rows(n, f):
    @pl.loop(0, n // STEP)
    def _(i):
        f(pl.ds(pl.multiple_of(i * STEP, STEP), STEP))


def _mid_fwd(total, put, ins, outs):
    x, g2 = ins
    xh_out, rs_out = outs
    n = total.shape[0]

    def f(r):
        h = x[r, :].astype(F32) + total[r, :]
        xc = h - jnp.mean(h, axis=-1, keepdims=True)
        rs = lax.rsqrt(jnp.mean(xc * xc, axis=-1, keepdims=True) + EPS)
        xh = xc * rs
        xh_out[r, :] = xh
        rs_out[r, :] = jnp.broadcast_to(rs, (rs.shape[0], rs_out.shape[1]))
        put(r, (xh * g2[...].astype(F32)).astype(BF))
    _rows(n, f)


def _lnb(dn, xh, rs, g):
    u = dn * g
    return rs * (u - jnp.mean(u, axis=-1, keepdims=True) - xh * jnp.mean(u * xh, axis=-1, keepdims=True))


def _mid_mlp(total, put, ins, outs):
    dy, g2, xh, rs = ins
    (dh_out,) = outs
    n = total.shape[0]

    def f(r):
        dh = dy[r, :].astype(F32) + _lnb(total[r, :], xh[r, :], rs[r, 0:1], g2[...].astype(F32))
        dh_out[r, :] = dh
        put(r, dh.astype(BF))
    _rows(n, f)


def _mid_in(total, put, ins, outs):
    x, g1, ms, dh = ins
    n = total.shape[0]

    def f(r):
        mu, rs = ms[r, 0:1], ms[r, 1:2]
        xh = (x[r, :].astype(F32) - mu) * rs
        dx = dh[r, :] + _lnb(total[r, :], xh, rs, g1[...].astype(F32))
        put(r, dx.astype(BF))
    _rows(n, f)


class _Layout:
    def __init__(self, n, t):
        self.n = n
        self.half, self.unit, self.b = t // 2, t // (2 * n), t // (2 * n * n)
        me = lax.axis_index("tp")
        c, chip = me % 2, me // 2
        y, x = chip // n, chip % n
        self.c = c
        self.f = f = (1 - c) * y + c * x
        self.s = s = (1 - c) * x + c * y

        def dev(f_, s_):
            return (((1 - c) * f_ + c * s_) * n + (1 - c) * s_ + c * f_) * 2 + c
        self.fr, self.fl = dev((f + 1) % n, s), dev((f + n - 1) % n, s)
        self.sr, self.sl = dev(f, (s + 1) % n), dev(f, (s + n - 1) % n)
        self.partner = me + 1 - 2 * c

    def row(self, s_, f_):
        return pl.multiple_of(self.c * self.half + s_ * self.unit + f_ * self.b, self.b)


def _remote(src, dst, ssem, rsem, to):
    return _Copy(lambda: pltpu.make_async_remote_copy(
        src_ref=src, dst_ref=dst, send_sem=ssem, recv_sem=rsem, device_id={"tp": to}, device_id_type=MESH))


def _core(n, trans, R, rows_of, late, mid, fill, consume, gather):
    L = _Layout(n, R["ag"].shape[0])
    half, unit, b, c, f, s = L.half, L.unit, L.b, L.c, L.f, L.s
    hb = b // 2
    l_ref, lo, lp, w, wp = R["l"], R["lo"], R["lp"], R["wv"], R["wpv"]
    pb, ra, rb, q, r2a, r2b, ag, tot = (R[k] for k in ("pb", "ra", "rb", "q", "r2a", "r2b", "ag", "tot"))
    d = ag.shape[1]
    lsem = R["lsem"]

    first = [pltpu.make_async_copy(R["w"], w, lsem.at[0]), pltpu.make_async_copy(R["wp"], wp, lsem.at[1]),
             pltpu.make_async_copy(l_ref.at[pl.ds(pl.multiple_of(c * half, half), half)], lo, lsem.at[2])]
    late = [pltpu.make_async_copy(R[a], R[z], lsem.at[4 + i]) for i, (a, z) in enumerate(late)]
    late.append(pltpu.make_async_copy(R[rows_of].at[pl.ds(L.row(s, f), b)], R["xv"], lsem.at[3]))
    for cp in first:
        cp.start()

    barrier = pltpu.get_barrier_semaphore()
    for p in (L.fr, L.fl, L.sr, L.sl, L.partner):
        pl.semaphore_signal(barrier, inc=1, device_id={"tp": p}, device_id_type=MESH)
    pl.semaphore_wait(barrier, 5)

    def blk(k):
        return (f + k) % n

    lx = _remote(l_ref.at[pl.ds(pl.multiple_of((1 - c) * half, half), half)], lp, R["sl"].at[0], R["sl"].at[1], L.partner)
    lx.start()
    for cp in late:
        cp.start()
    for cp in first:
        cp.wait()
    lx.wait_recv()

    dims = NT if trans else NN
    nt = 512

    def product(k):
        rows = pl.ds(pl.multiple_of(((s + OFFS[k]) % n) * unit, unit), unit)

        @pl.loop(0, d // nt)
        def _(j):
            cs = pl.ds(pl.multiple_of(j * nt, nt), nt)
            wa = w[cs, :] if trans else w[:, cs]
            wb = wp[cs, :] if trans else wp[:, cs]
            acc = lax.dot_general(lo[rows, :], wa, dims, preferred_element_type=F32)
            acc = acc + lax.dot_general(lp[rows, :], wb, dims, preferred_element_type=F32)
            acc = acc.astype(BF)
            for i in range(n):
                pb[k, i, :, cs] = acc[i * b:(i + 1) * b]

    def add_rows(dst, src, rows, off):
        def add(r):
            rd = pl.ds(pl.multiple_of(off + r.start, STEP), STEP)
            dst[rd, :] = (dst[rd, :].astype(F32) + src[r, :].astype(F32)).astype(BF)
        _rows(rows, add)

    s1, r1, s2, r2 = R["s1"], R["r1"], R["s2"], R["r2"]

    def c1a(k):
        o = pb.at[k, blk(2)]
        return (_remote(o.at[pl.ds(0, hb)], ra.at[k, 0], s1.at[k, 0], r1.at[k, 0], L.fr),
                _remote(o.at[pl.ds(hb, hb)], ra.at[k, 1], s1.at[k, 1], r1.at[k, 1], L.fl))

    def c1b(k):
        return (_remote(pb.at[k, blk(1)], rb.at[k, 0], s1.at[k, 2], r1.at[k, 2], L.fr),
                _remote(pb.at[k, blk(3)], rb.at[k, 1], s1.at[k, 3], r1.at[k, 3], L.fl))

    a2 = (_remote(q.at[0, pl.ds(0, hb)], r2a.at[0], s2.at[0], r2.at[0], L.sr),
          _remote(q.at[0, pl.ds(hb, hb)], r2a.at[1], s2.at[1], r2.at[1], L.sl))
    b2 = (_remote(q.at[1], r2b.at[0], s2.at[2], r2.at[2], L.sr),
          _remote(q.at[2], r2b.at[1], s2.at[3], r2.at[3], L.sl))

    def step_a(k):
        product(k)
        for cp in c1a(k):
            cp.start()

    def step_b(k):
        ca, cb = c1a(k), c1b(k)
        ca[0].wait_recv()
        add_rows(pb.at[k, blk(1)], ra.at[k, 0], hb, 0)
        cb[0].start()
        ca[1].wait_recv()
        add_rows(pb.at[k, blk(3)], ra.at[k, 1], hb, hb)
        cb[1].start()

    def step_c(k):
        for cp in c1b(k):
            cp.wait_recv()
        mine, l, r = pb.at[k, f], rb.at[k, 0], rb.at[k, 1]

        def add(i):
            q[k, i, :] = (mine[i, :].astype(F32) + l[i, :].astype(F32) + r[i, :].astype(F32)).astype(BF)
        _rows(b, add)

    def step_d(k):
        if k == 0:
            for cp in a2:
                cp.start()
        else:
            a2[k - 1].wait_recv()
            add_rows(q.at[k], r2a.at[k - 1], hb, (k - 1) * hb)
            b2[k - 1].start()

    def rest(_):
        for cp in late:
            cp.wait()

    _run("a0a1b0a2b1a3w0x0b2c0d0x1b3x2c1d1c2d2x3", a=step_a, b=step_b, c=step_c, d=step_d, w=rest, x=fill)
    for cp in c1b(3):
        cp.wait_recv()
    b2[0].wait_recv()
    b2[1].wait_recv()

    def final(r):
        tot[r, :] = (pb[3, f, r, :].astype(F32) + rb[3, 0, r, :].astype(F32) + rb[3, 1, r, :].astype(F32)
                     + r2b[0, r, :].astype(F32) + r2b[1, r, :].astype(F32))
    _rows(b, final)

    r0 = L.row(s, f)

    def put(r, v):
        ag[pl.ds(pl.multiple_of(r0 + r.start, STEP), r.size), :] = v
    mid(tot, put)

    gs, gr, hs, hr, ds, dr, osem = (R[k] for k in ("gs", "gr", "hs", "hr", "ds", "dr", "osem"))

    def gcopy(row_, off, size, ssem, rsem, to):
        v = ag.at[pl.ds(pl.multiple_of(row_ + off, hb), size)]
        return _remote(v, v, ssem, rsem, to)

    gS = (gcopy(r0, 0, b, gs.at[0], gr.at[0], L.sr), gcopy(r0, 0, b, gs.at[1], gr.at[1], L.sl),
          gcopy(L.row((s + n - 1) % n, f), 0, hb, gs.at[2], gr.at[2], L.sr),
          gcopy(L.row((s + 1) % n, f), hb, hb, gs.at[3], gr.at[3], L.sl))

    def urow(u, k):
        return L.row((s + GOFFS[u]) % n, blk(k))

    def gF(u):
        return (gcopy(urow(u, 0), 0, b, hs.at[u, 0], hr.at[u, 0], L.fr),
                gcopy(urow(u, 0), 0, b, hs.at[u, 1], hr.at[u, 1], L.fl),
                gcopy(urow(u, 3), 0, hb, hs.at[u, 2], hr.at[u, 2], L.fr),
                gcopy(urow(u, 1), hb, hb, hs.at[u, 3], hr.at[u, 3], L.fl))

    def pair(u, k):
        return gcopy(urow(u, k), 0, b, ds.at[u, k], dr.at[u, k], L.partner)

    def urows(u, i):
        core = c + i * (1 - 2 * c)
        return core * half + (((1 - i) * s + i * f + GOFFS[u]) % n) * unit

    def out(u, i):
        sl2 = pl.ds(pl.multiple_of(urows(u, i), unit), unit)
        return pltpu.make_async_copy(ag.at[sl2], R["g"].at[sl2], osem.at[2 * u + i])

    def f1(u):
        g = gF(u)
        g[0].start()
        g[1].start()
        pair(u, 0).start()

    def f2(u):
        g = gF(u)
        g[0].wait_recv()
        g[2].start()
        pair(u, 3).start()
        g[1].wait_recv()
        g[3].start()
        pair(u, 1).start()

    def f3(u):
        g = gF(u)
        g[2].wait_recv()
        g[3].wait_recv()
        pair(u, 2).start()
        if gather:
            out(u, 0).start()

    def use(u):
        for k in range(n):
            pair(u, k).wait_recv()
        if gather:
            out(u, 1).start()
        consume(u, lambda i: pl.multiple_of(urows(u, i), unit))

    ops = dict(s=lambda k: gS[k].start(), w=lambda k: gS[k].wait_recv(), f=f1, g=f2, h=f3, u=use)
    _run("s0s1f0w0s2w1s3g0f1f2h0u0", **ops)
    _run("g1w2w3f3g2h1u1g3h2u2h3u3", **ops)

    if gather:
        for u in range(n):
            out(u, 0).wait()
            out(u, 1).wait()
    lx.wait_send()
    for k in range(n):
        for cp in c1a(k) + c1b(k):
            cp.wait_send()
    for cp in a2 + b2 + gS:
        cp.wait_send()
    for u in range(n):
        for cp in gF(u):
            cp.wait_send()
        for k in range(n):
            pair(u, k).wait_send()


class _Stream:
    def __init__(self, srcs, factor, out, buf, stage, isem, osem, cuts):
        self.srcs, self.factor, self.out, self.buf, self.stage = srcs, factor, out, buf, stage
        self.isem, self.osem, self.cuts = isem, osem, cuts
        self.width = buf.shape[2]
        self.per = srcs[0].shape[1] // self.width
        self.n = self.per * len(srcs)
        assert cuts[-1] == self.n

    def load(self, i, go):
        sl = i % 2
        for a, src in enumerate(self.srcs):
            @pl.when(jnp.logical_and(i >= a * self.per, i < (a + 1) * self.per))
            def _():
                cs = pl.ds(pl.multiple_of((i - a * self.per) * self.width, self.width), self.width)
                go(pltpu.make_async_copy(src.at[:, cs], self.buf.at[sl], self.isem.at[sl]))

    def store(self, i):
        cs = pl.ds(pl.multiple_of((i % self.per) * self.width, self.width), self.width)
        return pltpu.make_async_copy(self.stage.at[i % 2], self.out.at[i // self.per, :, cs], self.osem.at[i % 2])

    def fill(self, site):
        lo, hi = ((0,) + self.cuts)[site], self.cuts[site]
        if site == 0:
            self.load(jnp.int32(0), lambda cp: cp.start())

        @pl.loop(lo, hi)
        def _(i):
            self.load(i, lambda cp: cp.wait())

            @pl.when(i + 1 < self.n)
            def _():
                self.load(i + 1, lambda cp: cp.start())

            @pl.when(i >= 2)
            def _():
                self.store(i - 2).wait()
            v = jnp.dot(self.factor[i // self.per], self.buf[i % 2], preferred_element_type=F32)
            self.stage[i % 2] = v.astype(BF)
            self.store(i).start()
        if hi == self.n:
            self.store(jnp.int32(self.n - 2)).wait()
            self.store(jnp.int32(self.n - 1)).wait()


_K = 0.7978845608028654


def _fwd_kernel(names, n, *refs):
    R = dict(zip(names, refs))
    dgs, dyb, dsem, osem2 = R["dgs"], R["dyb"], R["dsem"], R["lsem2"]
    rows = dyb.shape[1]
    tiles = dgs.shape[0] // rows
    cuts = (2, 4, 6, tiles)

    def load(i):
        return pltpu.make_async_copy(R["dy"].at[pl.ds(pl.multiple_of(i * rows, rows), rows)], dyb.at[i % 2], dsem.at[i % 2])

    def fill(site):
        if site == 0:
            load(jnp.int32(0)).start()

        @pl.loop(((0,) + cuts)[site], cuts[site])
        def _(i):
            load(i).wait()

            @pl.when(i + 1 < tiles)
            def _():
                load(i + 1).start()
            dgs[pl.ds(pl.multiple_of(i * rows, rows), rows), :] = lax.dot_general(
                dyb[i % 2], R["w2v"][...], NT, preferred_element_type=F32)

    def stores(i, r, w):
        return [pltpu.make_async_copy(R["sda"].at[i], R["da"].at[pl.ds(r, w)], osem2.at[0, i]),
                pltpu.make_async_copy(R["sgt"].at[i], R["lt"].at[0, :, pl.ds(r, w)], osem2.at[1, i]),
                pltpu.make_async_copy(R["sdt"].at[i], R["lt"].at[1, :, pl.ds(r, w)], osem2.at[2, i])]
    prev = []

    def consume(u, row):
        w = R["sda"].shape[1]

        @pl.loop(0, 2)
        def _(i):
            r = row(i)
            for p in prev[-1:]:
                for cp in stores(i, p(i), w):
                    cp.wait()
            a = jnp.dot(R["ag"][pl.ds(r, w), :], R["w1v"][...], preferred_element_type=F32)
            th = jnp.tanh(_K * (a + 0.044715 * (a * a * a)))
            cdf = 0.5 * (1.0 + th)
            slope = cdf + 0.5 * a * ((1.0 - th * th) * (_K * (1.0 + (3 * 0.044715) * (a * a))))
            gl = (a * cdf).astype(BF)
            da = (dgs[pl.ds(r, w), :] * slope).astype(BF)
            R["sda"][i] = da
            R["sgt"][i] = gl.T
            R["sdt"][i] = da.T
            for cp in stores(i, r, w):
                cp.start()
        prev.append(row)

    _core(n, False, R, "x", (("w2", "w2v"), ("w1", "w1v")),
          lambda tot, put: _mid_fwd(tot, put, (R["xv"], R["g2"]), (R["xh"], R["rs"])), fill, consume, True)
    for i in range(2):
        for cp in stores(i, prev[-1](i), R["sda"].shape[1]):
            cp.wait()


def _mlp_kernel(names, n, *refs):
    R = dict(zip(names, refs))
    st = _Stream((R["dy"], R["n2"]), R["ltv"], R["dw"], R["buf"], R["stage"], R["bsem"], R["tsem"], (7, 16, 21, 32))
    acc = R["acc"]
    d = acc.shape[1]
    w = R["ag"].shape[0] // (2 * n)
    nt = 512

    def consume(u, row):
        @pl.loop(0, 2)
        def _(i):
            r = row(i)
            do = lax.dot_general(R["ag"][pl.ds(r, w), :], R["wv0"][...], NT, preferred_element_type=F32)
            R["do"][pl.ds(r, w), :] = do.astype(BF)
            ot = R["ov"][pl.ds(r, w), :]

            @pl.loop(0, d // nt)
            def _(j):
                cs = pl.ds(pl.multiple_of(j * nt, nt), nt)
                v = lax.dot_general(ot, R["ag"][pl.ds(r, w), cs], TN, preferred_element_type=F32)
                acc[:, cs] = acc[:, cs] + v

    acc[...] = jnp.zeros_like(acc)
    _core(n, True, R, "dy", (("lt", "ltv"), ("wo", "wv0"), ("o", "ov")),
          lambda tot, put: _mid_mlp(tot, put, (R["xv"], R["g2"], R["xh"], R["rs"]), (R["dh"],)), st.fill, consume, False)
    R["dwo"][...] = acc[...].astype(BF)


def _in_kernel(names, n, *refs):
    R = dict(zip(names, refs))
    st = _Stream((R["n1"],), R["ltv"], R["dw"], R["buf"], R["stage"], R["bsem"], R["tsem"], (4, 8, 11, 16))
    _core(n, True, R, "x", (("lt", "ltv"),),
          lambda tot, put: _mid_in(tot, put, (R["xv"], R["g1"], R["ms"], R["dh"]), ()), st.fill,
          lambda u, row: None, True)


ANY, VM = pl.BlockSpec(memory_space=pl.ANY), pl.BlockSpec(memory_space=pltpu.VMEM)


def _exchange(tp, cid, kernel, flops, ins, outs, scratch):
    n = round((tp // 2) ** 0.5)
    assert n == 4 and n * n * 2 == tp
    l, w, wp = (ins[k][0] for k in ("l", "w", "wp"))
    t, kk = l.shape
    d = w.shape[0] * w.shape[1] // kk
    half, b = t // 2, t // tp
    dma = pltpu.SemaphoreType.DMA
    vm = pltpu.VMEM
    scratch = dict(
        lo=vm((half, kk), BF), lp=vm((half, kk), BF), wv=vm(w.shape, BF), wpv=vm(w.shape, BF),
        pb=vm((n, n, b, d), BF), ra=vm((n, 2, b // 2, d), BF), rb=vm((n, 2, b, d), BF), q=vm((n - 1, b, d), BF),
        r2a=vm((2, b // 2, d), BF), r2b=vm((2, b, d), BF), ag=vm((t, d), BF), tot=vm((b, d), F32), xv=vm((b, d), BF),
        lsem=dma((7,)), sl=dma((2,)), s1=dma((n, 4)), r1=dma((n, 4)), s2=dma((4,)), r2=dma((4,)),
        gs=dma((4,)), gr=dma((4,)), hs=dma((n, 4)), hr=dma((n, 4)), ds=dma((n, n)), dr=dma((n, n)), osem=dma((2 * n,)),
        **scratch)
    names = (*ins, *outs, *scratch)
    assert len(set(names)) == len(names)
    return pl.pallas_call(
        functools.partial(kernel, names, n),
        out_shape=[jax.ShapeDtypeStruct(s, dt) for s, dt, _ in outs.values()],
        in_specs=[sp for _, sp in ins.values()],
        out_specs=[sp for _, _, sp in outs.values()],
        scratch_shapes=list(scratch.values()),
        compiler_params=pltpu.CompilerParams(collective_id=cid, has_side_effects=True,
                                             vmem_limit_bytes=67043328),
        cost_estimate=pl.CostEstimate(flops=flops, bytes_accessed=t * d * 4, transcendentals=0),
        name=f"exchange{cid}",
    )(*(a for a, _ in ins.values()))


def _qkv_kernel(x, ms, g, w, n1, qkv):
    v = ((x[...].astype(F32) - ms[:, 0:1]) * ms[:, 1:2] * g[...].astype(F32)).astype(BF)
    n1[...] = v
    qkv[...] = jnp.dot(v, w[...], preferred_element_type=F32).astype(BF)


def _norm_qkv(x, ms, g, w):
    t, d = x.shape
    m, rows = w.shape[1], 256
    return pl.pallas_call(
        _qkv_kernel,
        grid=(t // rows,),
        in_specs=[pl.BlockSpec((rows, d), _down), pl.BlockSpec((rows, 2), _down),
                  pl.BlockSpec((1, d), lambda i: (0, 0)),
                  pl.BlockSpec((d, m), lambda i: (0, 0))],
        out_specs=[pl.BlockSpec((rows, d), _down), pl.BlockSpec((rows, m), _down)],
        out_shape=[jax.ShapeDtypeStruct((t, d), BF), jax.ShapeDtypeStruct((t, m), BF)],
        compiler_params=pltpu.CompilerParams(vmem_limit_bytes=LIMIT),
        cost_estimate=pl.CostEstimate(flops=2 * t * d * m, bytes_accessed=t * d * 4, transcendentals=0),
        name="norm_qkv",
    )(x, ms, g, w)


def solution(mesh):
    tp = mesh.shape["tp"]
    swap = [(i, i + 1 - 2 * (i % 2)) for i in range(tp)]

    rows, cols = P("dp"), P(None, "tp")

    def body(x, mu1, rs1, g1, g2, dy, wqkv, wo, w1, w2):
        hl, hd, d = wo.shape
        t = x.shape[0]
        side = round((tp // 2) ** 0.5)
        b = t // tp
        me = lax.axis_index("tp")
        c, chip = me % 2, me // 2
        yy, xx = chip // side, chip % side
        own = c * (t // 2) + ((1 - c) * (xx * side + yy) + c * (yy * side + xx)) * b
        wo2 = wo.reshape(hl * hd, d)
        wo_p = lax.ppermute(wo2, "tp", swap)
        w1_p = lax.ppermute(w1, "tp", swap)
        wqkv_p = lax.ppermute(wqkv, "tp", swap)

        ms = jnp.stack([mu1, rs1], axis=1)
        msr = lax.dynamic_slice_in_dim(ms, own, b, 0)
        g1r, g2r = g1[None, :], g2[None, :]
        dma, vm = pltpu.SemaphoreType.DMA, pltpu.VMEM
        n1, qkv = _norm_qkv(x, ms, g1r, wqkv)
        assert hl == 1
        o, lse = _attn_fwd(qkv, hd)
        m = w1.shape[1]
        unit = t // (2 * side)
        n2, xh2, rs2, da, lt = _exchange(
            tp, 0, _fwd_kernel, 8 * t * d * m,
            dict(l=(o, ANY), w=(wo2, ANY), wp=(wo_p, ANY), x=(x, ANY), g2=(g2r, VM),
                 dy=(dy, ANY), w2=(w2, ANY), w1=(w1, ANY)),
            dict(g=((t, d), BF, ANY), xh=((b, d), F32, VM), rs=((b, 128), F32, VM),
                 da=((t, m), BF, ANY), lt=((2, m, t), BF, ANY)),
            dict(w2v=vm(w2.shape, BF), w1v=vm(w1.shape, BF), dgs=vm((t, m), F32), dyb=vm((2, unit, d), BF),
                 sda=vm((2, unit, m), BF), sgt=vm((2, m, unit), BF), sdt=vm((2, m, unit), BF),
                 dsem=dma((2,)), lsem2=dma((3, 2))))
        dh1, dw, do, dwo = _exchange(
            tp, 1, _mlp_kernel, 8 * t * d * m,
            dict(l=(da, ANY), w=(w1, ANY), wp=(w1_p, ANY), g2=(g2r, VM), xh=(xh2, VM), rs=(rs2, VM),
                 dy=(dy, ANY), n2=(n2, ANY), lt=(lt, ANY), wo=(wo2, ANY), o=(o, ANY)),
            dict(dh=((b, d), F32, VM), dw=((2, m, d), BF, ANY), do=((t, hd), BF, VM), dwo=((hd, d), BF, VM)),
            dict(ltv=vm(lt.shape, BF), wv0=vm(wo2.shape, BF), ov=vm(o.shape, BF), acc=vm((hd, d), F32),
                 buf=vm((2, t, 256), BF), stage=vm((2, m, 256), BF), bsem=dma((2,)), tsem=dma((2,))))
        dqkv, lt2, dw2, dw1, dwo = _attn_bwd(qkv, do, lse, dw, dwo, hd)
        dwo = dwo.reshape(hl, hd, d)
        dx, dwt = _exchange(
            tp, 2, _in_kernel, 8 * t * d * m,
            dict(l=(dqkv, ANY), w=(wqkv, ANY), wp=(wqkv_p, ANY), x=(x, ANY), g1=(g1r, VM), ms=(msr, VM),
                 dh=(dh1, VM), n1=(n1, ANY), lt=(lt2, ANY)),
            dict(g=((t, d), BF, ANY), dw=((1, 3 * hd, d), BF, ANY)),
            dict(ltv=vm(lt2.shape, BF), buf=vm((2, t, 256), BF), stage=vm((2, 3 * hd, 256), BF),
                 bsem=dma((2,)), tsem=dma((2,))))
        dx, dwqkv = _finish(dx, dwt)
        return dx, dwqkv, dwo, dw1, dw2

    return jax.shard_map(
        body, mesh=mesh,
        in_specs=(rows, P("dp"), P("dp"), P(), P(), rows, cols, P("tp"), cols, P("tp")),
        out_specs=(rows, P("dp", "tp"), P(("dp", "tp")), P("dp", "tp"), P(("dp", "tp"))),
        check_vma=False)
```
